32 devices in a mesh: dp: 4 (over y, z), tp: 8 (over x, core).
Axes of the slice: x: 4, y: 2, z: 2, core: 2. Of those that a mesh axis runs over, the one named last changes fastest.
The devices are a block of a 4x4x8 slice.
Arguments:
- X: bfloat16 [8192, 4096], P('dp'), parts along dimension 0
- W: bfloat16 [4096, 32768], P(None, 'tp')
- labels: int32 [8192], P('dp'), parts along dimension 0
Outputs:
- output 1: float32 [4], P('dp'), parts along dimension 0
- output 2: bfloat16 [16384, 32768], P('dp', 'tp'), parts along dimension 0
- output 3: bfloat16 [8192, 4096], P('dp'), parts along dimension 0
There are 4 independent parts. The reference program is written for one: setup_inputs(seed, part) draws one part's arguments, and reference() takes and returns one part's arrays. A program takes and returns all parts, laid end to end along the dimension named above; an argument that names none is the same for every part.
All inputs are finite; a program needn't handle non-finite values.
Results may differ from the reference program's by a relative error of at most 0.001.
Values are sent between devices in bfloat16 or wider.
A program may use at most 768 MiB of HBM per device.

```python
import math

import jax
import jax.numpy as jnp
from jax import lax

T = 2048
H = 4096
V = 32768


def setup_inputs(seed: int = 0, part: int = 0) -> dict:
    key = jax.random.PRNGKey(seed)
    kshared, kpart = jax.random.split(key)
    kp = jax.random.fold_in(kpart, part)
    kx, kl, kc, ku, kv, kg = jax.random.split(kp, 6)
    nb = 4
    Wf = jax.random.normal(kshared, (H, V), jnp.float32) * H ** -0.5
    kl1, kl2 = jax.random.split(jax.random.fold_in(kl, 7))
    la = jax.random.randint(kl1, (T,), 0, V // 16, jnp.int32)
    lb = jax.random.randint(kl2, (T,), 0, V, jnp.int32)
    labels = jnp.where(jnp.arange(T) % 2 == 0, la, lb)
    cols = jax.random.randint(kc, (T, nb), 0, V, jnp.int32)
    amp = math.log(V) + jax.random.uniform(ku, (T, nb), jnp.float32, 0.0, 2.5)
    amp_label = (math.log(V) + jax.random.uniform(kv, (T,), jnp.float32, -2.0, 2.0)
                 + jax.random.uniform(kg, (), jnp.float32, -1.0, 1.0))
    X = jax.random.normal(kx, (T, H), jnp.float32)
    for k in range(nb):
        X = X + amp[:, k:k + 1] * Wf[:, cols[:, k]].T
    X = X + amp_label[:, None] * Wf[:, labels].T
    return {'X': X.astype(jnp.bfloat16), 'W': Wf.astype(jnp.bfloat16), 'labels': labels}


def reference(X, W, labels):
    VC = min(V, 2048)
    nb = V // VC
    Wb = W.reshape(H, nb, VC).transpose(1, 0, 2)
    offs = jnp.arange(nb, dtype=jnp.int32) * VC
    cols = jnp.arange(VC, dtype=jnp.int32)

    def stats(a):
        w, off = a
        z = jnp.dot(X, w, preferred_element_type=jnp.float32)
        m = z.max(axis=1)
        s = jnp.exp(z - m[:, None]).sum(axis=1)
        hit = (cols[None, :] + off) == labels[:, None]
        t = jnp.where(hit, z, 0.0).sum(axis=1)
        return m, s, t

    m, s, t = lax.map(stats, (Wb, offs))
    M = m.max(axis=0)
    S = (s * jnp.exp(m - M[None, :])).sum(axis=0)
    zt = t.sum(axis=0)
    L = jnp.mean(M + jnp.log(S) - zt).reshape(1)

    def back(dx, a):
        w, off = a
        z = jnp.dot(X, w, preferred_element_type=jnp.float32)
        hit = (cols[None, :] + off) == labels[:, None]
        g = ((jnp.exp(z - M[:, None]) / S[:, None] - hit.astype(jnp.float32)) / T).astype(jnp.bfloat16)
        dw = jnp.dot(X.T, g, preferred_element_type=jnp.float32).astype(jnp.bfloat16)
        dx = dx + jnp.dot(g, w.T, preferred_element_type=jnp.float32)
        return dx, dw

    dx, dWb = lax.scan(back, jnp.zeros((T, H), jnp.float32), (Wb, offs))
    dW = dWb.transpose(1, 0, 2).reshape(H, V)
    return (L, dW, dx.astype(jnp.bfloat16))
```

```python
import functools
import math

import jax
import jax.numpy as jnp
from jax import lax
from jax.experimental import pallas as pl
from jax.experimental.pallas import tpu as pltpu
from jax.sharding import PartitionSpec as P

F32 = jnp.float32
BF16 = jnp.bfloat16
MESH = pl.DeviceIdType.MESH

NS = 4
NSL = 8
LANES = 128


def _main(n, nb, T, x_hbm, w_hbm, lab_hbm, g_hbm, dxs_hbm, loss_ref,
          w_v, z_v, x_v, g_v, lab_v, m_s, s_s, t_s, mrep, rrep,
          st_send, st_v, dxb, d2d, r1, r2, s1, s2, fin, o_v,
          w_sem, x_sem, lab_sem, g_sem, st_ssem, st_rsem,
          d2d_ssem, d2d_rsem, s1_ssem, r1_rsem, s2_ssem, r2_rsem, o_sem):
    nch = n // 2
    R = x_v.shape[2]
    BT = n * R
    H, Vl = w_v.shape
    TN = Vl // NS
    TH = H // NS
    inv_t = 1.0 / T
    me = lax.axis_index("tp")
    p, c = me // 2, me % 2
    co = 1 - c
    pr, plf, po = (p + 1) % nch, (p + nch - 1) % nch, (p + 2) % nch
    right, left, partner = {"tp": pr * 2 + c}, {"tp": plf * 2 + c}, {"tp": p * 2 + co}

    def w_copy(j):
        cols = pl.ds(pl.multiple_of(j * TN, TN), TN)
        return pltpu.make_async_copy(w_hbm.at[:, cols], w_v.at[:, cols], w_sem.at[j])

    def rows_of(b):
        return pl.ds(pl.multiple_of(b * R, R), R)

    def x_copy(b):
        return pltpu.make_async_copy(x_hbm.at[:, rows_of(b), :], x_v.at[b % 2], x_sem.at[b % 2])

    def lab_copy(b):
        return pltpu.make_async_copy(lab_hbm.at[:, rows_of(b), :], lab_v.at[b % 3], lab_sem.at[b % 3])

    def g_copy(b):
        return pltpu.make_async_copy(g_v, g_hbm.at[:, rows_of(b), :], g_sem)

    def st_copy(b, d):
        dev = (me + d) % n
        return pltpu.make_async_remote_copy(
            st_send.at[b % 2], st_v.at[b % 2, me], st_ssem.at[b % 2, d], st_rsem.at[b % 2, d],
            device_id={"tp": dev}, device_id_type=MESH)

    def d2d_copy(u):
        return pltpu.make_async_remote_copy(
            dxb.at[u % 2, :, co], d2d.at[u % NSL], d2d_ssem.at[u % 2], d2d_rsem.at[u % NSL],
            device_id=partner, device_id_type=MESH)

    hr = R // 2

    def rs1_copy(u, d):
        return pltpu.make_async_remote_copy(
            s1.at[u % 4, pl.ds(d * hr, hr)], r1.at[u % NSL, d],
            s1_ssem.at[u % 4, d], r1_rsem.at[u % NSL, d],
            device_id=right if d == 0 else left, device_id_type=MESH)

    def rs2_copy(u, d):
        return pltpu.make_async_remote_copy(
            s2.at[u % NSL, d], r2.at[u % NSL, d], s2_ssem.at[u % NSL, d], r2_rsem.at[u % NSL, d],
            device_id=right if d == 0 else left, device_id_type=MESH)

    def o_copy(u):
        b, s = u // NS, u % NS
        return pltpu.make_async_copy(
            o_v.at[u % 2],
            dxs_hbm.at[rows_of(b), pl.ds(pl.multiple_of(s * TH, TH), TH)],
            o_sem.at[u % 2])

    def u1(u):
        d2d_copy(u).wait_recv()
        k, kd = u % 2, u % NSL

        @pl.when(u >= 4)
        def _():
            for d in range(2):
                rs1_copy(u - 4, d).wait_send()

        @pl.when(u >= NSL)
        def _():
            for d in range(2):
                rs2_copy(u - NSL, d).wait_send()
        s1[u % 4] = dxb[k, po, c] + d2d[kd, po]
        for d in range(2):
            rs1_copy(u, d).start()
        s2[kd, 0] = dxb[k, pr, c] + d2d[kd, pr]
        s2[kd, 1] = dxb[k, plf, c] + d2d[kd, plf]
        fin[kd] = dxb[k, p, c] + d2d[kd, p]

    def u2(u):
        kd = u % NSL
        for d in range(2):
            rs1_copy(u, d).wait_recv()
            half = pl.ds(d * hr, hr)
            s2[kd, d, half] = s2[kd, d, half] + r1[kd, d]
            rs2_copy(u, d).start()

    def u3(u):
        kd = u % NSL
        for d in range(2):
            rs2_copy(u, d).wait_recv()

        @pl.when(u >= 2)
        def _():
            o_copy(u - 2).wait()
        o_v[u % 2] = (fin[kd] + r2[kd, 0] + r2[kd, 1]).astype(BF16)
        o_copy(u).start()

    def comm_z(i, j):
        @pl.when(jnp.logical_and(j == 0, i >= 2))
        def _():
            u1((i - 2) * NS + 3)

        @pl.when(jnp.logical_and(j == 0, i >= 3))
        def _():
            u3((i - 3) * NS + 3)

        @pl.when(i >= 2)
        def _():
            u2((i - 2) * NS + j)

    def comm_d(i, s):
        @pl.when(s >= 1)
        def _():
            u1((i - 1) * NS + s - 1)

        @pl.when(jnp.logical_and(s >= 1, i >= 2))
        def _():
            u3((i - 2) * NS + s - 1)

    lane = lax.broadcasted_iota(jnp.int32, (BT, LANES), 1)

    def z_tile(b, j):
        xs = x_v[b % 2].reshape(BT, H)
        lab = lab_v[b % 3].reshape(BT, LANES)
        sub = TN // 2
        for q in range(2):
            base = pl.multiple_of(j * TN + q * sub, sub)
            z = jnp.dot(xs, w_v[:, pl.ds(base, sub)], preferred_element_type=F32)
            z_v[b % 2, :, pl.ds(base, sub)] = z
            zs = [z[:, k * LANES:(k + 1) * LANES] for k in range(sub // LANES)]
            m_old = m_s[...]
            m_new = functools.reduce(jnp.maximum, zs, m_old)
            acc = s_s[...] * jnp.exp(m_old - m_new)
            tgt = t_s[...]
            for k, zk in enumerate(zs):
                acc = acc + jnp.exp(zk - m_new)
                tgt = tgt + jnp.where(lab == lane + (base + k * LANES), zk, 0.0)
            m_s[...] = m_new
            s_s[...] = acc
            t_s[...] = tgt

    def g_tile(b, j):
        lab = lab_v[b % 3].reshape(BT, LANES)
        for k in range(TN // LANES):
            base = pl.multiple_of(j * TN + k * LANES, LANES)
            z = z_v[b % 2, :, pl.ds(base, LANES)]
            pr_ = jnp.exp(z - mrep[...]) * rrep[...]
            hit = jnp.where(lab == lane + base, 1.0, 0.0)
            g = ((pr_ - hit) * inv_t).astype(BF16)
            g_v[:, :, pl.ds(base, LANES)] = g.reshape(n, R, LANES)

    def stats_init():
        m_s[...] = jnp.full((BT, LANES), -jnp.inf, F32)
        s_s[...] = jnp.zeros((BT, LANES), F32)
        t_s[...] = jnp.zeros((BT, LANES), F32)

    def stats_send(b):
        ml = m_s[...]
        m = jnp.max(ml, axis=1, keepdims=True)
        s = jnp.sum(s_s[...] * jnp.exp(ml - m), axis=1, keepdims=True)
        t = jnp.sum(t_s[...], axis=1, keepdims=True)
        a = jnp.where(lane == 0, m, jnp.where(lane == 1, s, t))
        a = a.T[0:8]
        st_send[b % 2] = a
        st_v[b % 2, me] = a
        for d in range(1, n):
            st_copy(b, d).start()

    def stats_recv(b):
        k = b % 2
        for d in range(1, n):
            st_copy(b, d).wait()
        ms = st_v[k, :, 0, :]
        m = jnp.max(ms, axis=0, keepdims=True)
        s = jnp.sum(st_v[k, :, 1, :] * jnp.exp(ms - m), axis=0, keepdims=True)
        t = jnp.sum(st_v[k, :, 2, :], axis=0, keepdims=True)
        loss_ref[...] += m + jnp.log(s) - t
        row = lax.broadcasted_iota(jnp.int32, (LANES, BT), 0)
        a = jnp.where(row == 0, m, 1.0 / s).T
        mrep[...] = jnp.broadcast_to(a[:, 0:1], (BT, LANES))
        rrep[...] = jnp.broadcast_to(a[:, 1:2], (BT, LANES))

    def d_tile(b, s):
        u = b * NS + s

        @pl.when(u >= 2)
        def _():
            d2d_copy(u - 2).wait_send()
        gs = g_v[...].reshape(BT, H if False else Vl)
        dx = lax.dot_general(gs, w_v[pl.ds(pl.multiple_of(s * TH, TH), TH), :],
                             (((1,), (1,)), ((), ())), preferred_element_type=F32)
        dxb[u % 2] = dx.reshape(nch, 2, R, TH)
        d2d_copy(u).start()

    for j in range(NS):
        w_copy(j).start()
        if j == 0:
            x_copy(0).start()
            lab_copy(0).start()
            lab_copy(1).start()
            x_copy(1).start()
    bar = pltpu.get_barrier_semaphore()
    for d in range(1, n):
        pl.semaphore_signal(bar, inc=1, device_id={"tp": (me + d) % n}, device_id_type=MESH)
    pl.semaphore_wait(bar, n - 1)

    loss_ref[...] = jnp.zeros_like(loss_ref)
    stats_init()
    x_copy(0).wait()
    lab_copy(0).wait()

    @pl.loop(0, NS)
    def _(j):
        w_copy(j).wait()
        z_tile(0, j)
    stats_send(0)

    @pl.loop(1, nb)
    def _(i):
        x_copy(i).wait()
        lab_copy(i).wait()
        stats_recv(i - 1)
        stats_init()

        @pl.when(i >= 2)
        def _():
            g_copy(i - 2).wait()

        @pl.when(i + 1 < nb)
        def _():
            x_copy(i + 1).start()
            lab_copy(i + 1).start()

        @pl.loop(0, NS)
        def _(j):
            comm_z(i, j)
            z_tile(i, j)
            g_tile(i - 1, j)
        stats_send(i)
        g_copy(i - 1).start()

        @pl.loop(0, NS)
        def _(s):
            comm_d(i, s)
            d_tile(i - 1, s)

    stats_recv(nb - 1)
    g_copy(nb - 2).wait()

    @pl.loop(0, NS)
    def _(j):
        comm_z(nb, j)
        g_tile(nb - 1, j)
    g_copy(nb - 1).start()

    @pl.loop(0, NS)
    def _(s):
        comm_d(nb, s)
        d_tile(nb - 1, s)

    nu = nb * NS

    @pl.loop(0, NS)
    def _(j):
        comm_z(nb + 1, j)

    @pl.loop(0, NS)
    def _(j):
        u3((nb - 1) * NS + j)

    for u in range(nu - 2, nu):
        d2d_copy(u).wait_send()
        o_copy(u).wait()
    for u in range(nu - 4, nu):
        for d in range(2):
            rs1_copy(u, d).wait_send()
    for u in range(nu - NSL, nu):
        for d in range(2):
            rs2_copy(u, d).wait_send()
    g_copy(nb - 1).wait()


def _dw(x_ref, g_ref, o_ref):
    o_ref[...] = lax.dot_general(x_ref[...], g_ref[...], (((0,), (0,)), ((), ())),
                                 preferred_element_type=F32).astype(BF16)


def solution(mesh):
    n = mesh.shape["tp"]

    def local(X, W, labels):
        T, H = X.shape
        Vl = W.shape[1]
        own = T // n
        R = 32
        nb = own // R
        BT = n * R
        TH = H // NS
        off = lax.axis_index("tp") * Vl
        lab = jnp.broadcast_to((labels - off)[:, None], (T, LANES)).reshape(n, own, LANES)
        hbm = pl.BlockSpec(memory_space=pl.ANY)
        vm = pltpu.VMEM
        dma = pltpu.SemaphoreType.DMA
        flops = 4 * T * H * Vl
        g, dxs, loss = pl.pallas_call(
            functools.partial(_main, n, nb, T),
            out_shape=(jax.ShapeDtypeStruct((n, own, Vl), BF16),
                       jax.ShapeDtypeStruct((own, H), BF16),
                       jax.ShapeDtypeStruct((1, BT), F32)),
            in_specs=[hbm, hbm, hbm],
            out_specs=(hbm, hbm, pl.BlockSpec(memory_space=pltpu.VMEM)),
            scratch_shapes=[
                vm((H, Vl), BF16), vm((2, BT, Vl), F32), vm((2, n, R, H), BF16),
                vm((n, R, Vl), BF16), vm((3, n, R, LANES), jnp.int32),
                vm((BT, LANES), F32), vm((BT, LANES), F32), vm((BT, LANES), F32),
                vm((BT, LANES), F32), vm((BT, LANES), F32),
                vm((2, 8, BT), F32), vm((2, n, 8, BT), F32),
                vm((2, n // 2, 2, R, TH), F32), vm((NSL, n // 2, R, TH), F32),
                vm((NSL, 2, R // 2, TH), F32), vm((NSL, 2, R, TH), F32),
                vm((4, R, TH), F32), vm((NSL, 2, R, TH), F32), vm((NSL, R, TH), F32),
                vm((2, R, TH), BF16),
                dma((NS,)), dma((2,)), dma((3,)), dma, dma((2, n)), dma((2, n)),
                dma((2,)), dma((NSL,)), dma((4, 2)), dma((NSL, 2)), dma((NSL, 2)),
                dma((NSL, 2)), dma((2,)),
            ],
            compiler_params=pltpu.CompilerParams(
                collective_id=0, has_side_effects=True, vmem_limit_bytes=67043328),
            cost_estimate=pl.CostEstimate(flops=flops, bytes_accessed=2 * (H * Vl + T * (H + Vl)),
                                          transcendentals=2 * T * Vl),
            name="head_main",
        )(X.reshape(n, own, H), W, lab)
        G = g.reshape(T, Vl)
        dX = lax.all_gather(dxs, "tp", axis=0, tiled=True)
        th, tv = 1024, 1024
        dW = pl.pallas_call(
            _dw,
            out_shape=jax.ShapeDtypeStruct((H, Vl), BF16),
            grid=(Vl // tv, H // th),
            in_specs=[pl.BlockSpec((T, th), lambda v, h: (0, h)),
                      pl.BlockSpec((T, tv), lambda v, h: (0, v))],
            out_specs=pl.BlockSpec((th, tv), lambda v, h: (h, v)),
            compiler_params=pltpu.CompilerParams(vmem_limit_bytes=48 * 1024 * 1024),
            cost_estimate=pl.CostEstimate(flops=2 * T * H * Vl,
                                          bytes_accessed=2 * (H * Vl + T * (H + Vl)),
                                          transcendentals=0),
            name="head_dw",
        )(X, G)
        L = (jnp.sum(loss) / T).reshape(1)
        return L, dW, dX

    return jax.shard_map(local, mesh=mesh,
                         in_specs=(P('dp', None), P(None, 'tp'), P('dp')),
                         out_specs=(P('dp'), P('dp', 'tp'), P('dp', None)),
                         check_vma=False)
```

```python
import functools
import math

import jax
import jax.numpy as jnp
from jax import lax
from jax.experimental import pallas as pl
from jax.experimental.pallas import tpu as pltpu
from jax.sharding import PartitionSpec as P

F32 = jnp.float32
BF16 = jnp.bfloat16
MESH = pl.DeviceIdType.MESH

NS = 4
NSL = 8
LANES = 128
TD = 512
NT = 6


def _main(n, nb, T, x_hbm, w_hbm, lab_hbm, g_hbm, dxf_hbm, dw1_hbm, loss_ref,
          lab_v, m_s, s_s, t_s, mrep, rrep,
          st_send, st_v, dxb, d2d, r1, r2, s1, s2, fin, o_v,
          w_sem, x_sem, lab_sem, g_sem, st_ssem, st_rsem,
          d2d_ssem, d2d_rsem, s1_ssem, r1_rsem, s2_ssem, r2_rsem, o_sem,
          ag_ssem, ag_rsem, xt_sem, gt_sem, ot_sem):
    nch = n // 2
    own = x_hbm.shape[1]
    R = lab_v.shape[2]
    BT = n * R
    H, Vl = w_hbm.shape
    TN = Vl // NS
    TH = H // NS
    inv_t = 1.0 / T
    me = lax.axis_index("tp")
    p, c = me // 2, me % 2
    co = 1 - c
    pr, plf, po = (p + 1) % nch, (p + nch - 1) % nch, (p + 2) % nch
    right, left, partner = {"tp": pr * 2 + c}, {"tp": plf * 2 + c}, {"tp": p * 2 + co}

    def rows_of(b):
        return pl.ds(pl.multiple_of(b * R, R), R)

    def lab_copy(b):
        return pltpu.make_async_copy(lab_hbm.at[:, rows_of(b), :], lab_v.at[b % 3], lab_sem.at[b % 3])

    def st_copy(b, d):
        dev = (me + d) % n
        return pltpu.make_async_remote_copy(
            st_send.at[b % 2], st_v.at[b % 2, me], st_ssem.at[b % 2, d], st_rsem.at[b % 2, d],
            device_id={"tp": dev}, device_id_type=MESH)

    def d2d_copy(u):
        return pltpu.make_async_remote_copy(
            dxb.at[u % 3, :, co], d2d.at[u % NSL], d2d_ssem.at[u % 3], d2d_rsem.at[u % NSL],
            device_id=partner, device_id_type=MESH)

    hr = R // 2

    def rs1_copy(u, d):
        return pltpu.make_async_remote_copy(
            s1.at[u % 4, pl.ds(d * hr, hr)], r1.at[u % NSL, d],
            s1_ssem.at[u % 4, d], r1_rsem.at[u % NSL, d],
            device_id=right if d == 0 else left, device_id_type=MESH)

    def rs2_copy(u, d):
        return pltpu.make_async_remote_copy(
            s2.at[u % NSL, d], r2.at[u % NSL, d], s2_ssem.at[u % NSL, d], r2_rsem.at[u % NSL, d],
            device_id=right if d == 0 else left, device_id_type=MESH)

    def o_copy(u):
        b, s = u // NS, u % NS
        return pltpu.make_async_copy(
            o_v.at[s], dxf_hbm.at[me, rows_of(b), pl.ds(pl.multiple_of(s * TH, TH), TH)],
            o_sem.at[s])

    opp = po * 2 + c
    qr, ql = pr * 2 + c, plf * 2 + c

    def ag_copy(kind, k, owner, lo, rows, dev):
        r = pl.ds(pl.multiple_of(k * R + lo, rows), rows)
        return pltpu.make_async_remote_copy(
            dxf_hbm.at[owner, r], dxf_hbm.at[owner, r], ag_ssem.at[kind, k], ag_rsem.at[kind, k],
            device_id=dev, device_id_type=MESH)

    def ag_all(k):
        args = [(me, 0, R, right), (me, 0, R, left), (me, 0, R, partner),
                (ql, 0, hr, right), (qr, hr, hr, left),
                (ql, 0, R, partner), (qr, 0, R, partner), (opp, 0, R, partner)]
        return [functools.partial(ag_copy, i, k, *x) for i, x in enumerate(args)]

    def ag_a(k):
        cs = ag_all(k)
        for i in (0, 1, 2):
            cs[i]().start()

    def ag_b(k):
        cs = ag_all(k)
        for i in (0, 1):
            cs[i]().wait_recv()
        for i in (3, 4, 5, 6):
            cs[i]().start()

    def ag_c(k):
        cs = ag_all(k)
        for i in (3, 4):
            cs[i]().wait_recv()
        cs[7]().start()

    def ag_end(k):
        cs = ag_all(k)
        for i in (2, 5, 6, 7):
            cs[i]().wait_recv()
        for cp in cs:
            cp().wait_send()

    def u1(u):
        d2d_copy(u).wait_recv()
        k, kd = u % 3, u % NSL

        @pl.when(u >= 4)
        def _():
            for d in range(2):
                rs1_copy(u - 4, d).wait_send()

        @pl.when(u >= NSL)
        def _():
            for d in range(2):
                rs2_copy(u - NSL, d).wait_send()
        s1[u % 4] = dxb[k, po, c] + d2d[kd, po]
        for d in range(2):
            rs1_copy(u, d).start()
        s2[kd, 0] = dxb[k, pr, c] + d2d[kd, pr]
        s2[kd, 1] = dxb[k, plf, c] + d2d[kd, plf]
        fin[kd] = dxb[k, p, c] + d2d[kd, p]

    def u2(u):
        kd = u % NSL
        for d in range(2):
            rs1_copy(u, d).wait_recv()
            half = pl.ds(d * hr, hr)
            s2[kd, d, half] = s2[kd, d, half] + r1[kd, d]
            rs2_copy(u, d).start()

    def u3(u):
        kd = u % NSL
        for d in range(2):
            rs2_copy(u, d).wait_recv()
        o_v[u % NS] = (fin[kd] + r2[kd, 0] + r2[kd, 1]).astype(BF16)
        o_copy(u).start()

    def when(cond):
        return pl.when(cond)

    def o_wait(b):
        for s in range(NS):
            o_copy(b * NS + s).wait()

    def comm_z(i, j):
        @when(jnp.logical_and(j < 2, i >= 2))
        def _():
            u1((i - 2) * NS + 2 + j)

        @when(jnp.logical_and(j < 3, i >= 3))
        def _():
            u3((i - 3) * NS + 1 + j)

        @when(jnp.logical_and(j >= 2, i >= 2))
        def _():
            u2((i - 2) * NS + j - 2)

    def comm_d(i, s):
        @when(jnp.logical_and(s < 2, i >= 2))
        def _():
            u2((i - 2) * NS + 2 + s)

        @when(s >= 2)
        def _():
            u1((i - 1) * NS + s - 2)

        @when(jnp.logical_and(s == 3, i >= 2))
        def _():
            u3((i - 2) * NS)

        @when(jnp.logical_and(s == 2, i >= 3))
        def _():
            o_wait(i - 3)

        @when(jnp.logical_and(s == 2, jnp.logical_and(i >= 5, i % 2 == 1)))
        def _():
            ag_c((i - 5) // 2)

        @when(jnp.logical_and(s == 2, jnp.logical_and(i >= 3, i % 2 == 1)))
        def _():
            ag_a((i - 3) // 2)

        @when(jnp.logical_and(s == 2, jnp.logical_and(i >= 4, i % 2 == 0)))
        def _():
            ag_b((i - 4) // 2)

    lane = lax.broadcasted_iota(jnp.int32, (BT, LANES), 1)

    bar = pltpu.get_barrier_semaphore()
    for d in range(1, n):
        pl.semaphore_signal(bar, inc=1, device_id={"tp": (me + d) % n}, device_id_type=MESH)
    pl.semaphore_wait(bar, n - 1)

    def phase1(w_v, z_v, x_v, g_v):
        def w_copy(j):
            cols = pl.ds(pl.multiple_of(j * TN, TN), TN)
            return pltpu.make_async_copy(w_hbm.at[:, cols], w_v.at[:, cols], w_sem.at[j])

        def x_copy(b):
            return pltpu.make_async_copy(x_hbm.at[:, rows_of(b), :], x_v.at[b % 2], x_sem.at[b % 2])

        def g_copy(b):
            return pltpu.make_async_copy(g_v, g_hbm.at[:, rows_of(b), :], g_sem)

        def z_tile(b, j):
            cols = pl.ds(pl.multiple_of(j * TN, TN), TN)
            z_v[:, cols] = jnp.dot(x_v[b % 2].reshape(BT, H), w_v[:, cols],
                                          preferred_element_type=F32)

        def stat_tile(b, j):
            for r in range(0, BT, 16):
                rows = pl.ds(r, 16)
                lab = lab_v[b % 3].reshape(BT, LANES)[r:r + 16]
                ln = lane[r:r + 16]
                zs = [z_v[rows, pl.ds(pl.multiple_of(j * TN + k * LANES, LANES), LANES)]
                      for k in range(TN // LANES)]
                m_old = m_s[rows]
                m_new = functools.reduce(jnp.maximum, zs, m_old)
                acc = s_s[rows] * jnp.exp(m_old - m_new)
                tgt = t_s[rows]
                for k, zk in enumerate(zs):
                    acc = acc + jnp.exp(zk - m_new)
                    tgt = tgt + jnp.where(lab == ln + (j * TN + k * LANES), zk, 0.0)
                m_s[rows] = m_new
                s_s[rows] = acc
                t_s[rows] = tgt

        def g_tile(b, j):
            rb = 2 * R
            for r in range(0, BT, rb):
                rows = pl.ds(r, rb)
                lab = lab_v[b % 3].reshape(BT, LANES)[r:r + rb]
                ln = lane[r:r + rb]
                mm, rr = mrep[rows], rrep[rows]
                for k in range(TN // LANES):
                    base = pl.multiple_of(j * TN + k * LANES, LANES)
                    z = z_v[rows, pl.ds(base, LANES)]
                    e = jnp.exp(z - mm) * rr
                    g = (e - jnp.where(lab == ln + base, 1.0, 0.0)) * inv_t
                    g_v[pl.ds(r // R, rb // R), :, pl.ds(base, LANES)] = (
                        g.astype(BF16).reshape(rb // R, R, LANES))

        def stats_init():
            m_s[...] = jnp.full((BT, LANES), -jnp.inf, F32)
            s_s[...] = jnp.zeros((BT, LANES), F32)
            t_s[...] = jnp.zeros((BT, LANES), F32)

        def stats_send(b):
            ml = m_s[...]
            m = jnp.max(ml, axis=1, keepdims=True)
            s = jnp.sum(s_s[...] * jnp.exp(ml - m), axis=1, keepdims=True)
            t = jnp.sum(t_s[...], axis=1, keepdims=True)
            a = jnp.where(lane == 0, m, jnp.where(lane == 1, s, t))
            a = a.T[0:8]
            st_send[b % 2] = a
            st_v[b % 2, me] = a
            for d in range(1, n):
                st_copy(b, d).start()

        def stats_recv(b):
            k = b % 2
            for d in range(1, n):
                st_copy(b, d).wait()
            ms = st_v[k, :, 0, :]
            m = jnp.max(ms, axis=0, keepdims=True)
            s = jnp.sum(st_v[k, :, 1, :] * jnp.exp(ms - m), axis=0, keepdims=True)
            t = jnp.sum(st_v[k, :, 2, :], axis=0, keepdims=True)
            loss_ref[...] += m + jnp.log(s) - t
            row = lax.broadcasted_iota(jnp.int32, (LANES, BT), 0)
            a = jnp.where(row == 0, m, 1.0 / s).T
            mrep[...] = jnp.broadcast_to(a[:, 0:1], (BT, LANES))
            rrep[...] = jnp.broadcast_to(a[:, 1:2], (BT, LANES))

        def d_tile(b, s):
            u = b * NS + s

            @pl.when(u >= 3)
            def _():
                d2d_copy(u - 3).wait_send()
            gs = g_v[...].reshape(BT, Vl)
            dx = lax.dot_general(gs, w_v[pl.ds(pl.multiple_of(s * TH, TH), TH), :],
                                 (((1,), (1,)), ((), ())), preferred_element_type=F32)
            dxb[u % 3] = dx.reshape(nch, 2, R, TH)
            d2d_copy(u).start()

        for j in range(NS):
            w_copy(j).start()
            if j == 0:
                x_copy(0).start()
                lab_copy(0).start()
                lab_copy(1).start()
                x_copy(1).start()
        loss_ref[...] = jnp.zeros_like(loss_ref)
        stats_init()
        x_copy(0).wait()
        lab_copy(0).wait()

        @pl.loop(0, NS)
        def _(j):
            w_copy(j).wait()
            z_tile(0, j)

        @pl.loop(0, NS)
        def _(j):
            stat_tile(0, j)
        stats_send(0)

        @pl.loop(1, nb)
        def _(i):
            x_copy(i).wait()
            lab_copy(i).wait()
            stats_recv(i - 1)
            stats_init()

            @pl.when(i >= 2)
            def _():
                g_copy(i - 2).wait()

            @pl.when(i + 1 < nb)
            def _():
                x_copy(i + 1).start()
                lab_copy(i + 1).start()

            @pl.loop(0, NS)
            def _(j):
                comm_z(i, j)

                @pl.when(j > 0)
                def _():
                    stat_tile(i, j - 1)
                g_tile(i - 1, j)
                z_tile(i, j)
            stat_tile(i, NS - 1)
            stats_send(i)
            g_copy(i - 1).start()

            @pl.loop(0, NS)
            def _(s):
                comm_d(i, s)
                d_tile(i - 1, s)

        stats_recv(nb - 1)
        g_copy(nb - 2).wait()

        @pl.loop(0, NS)
        def _(j):
            comm_z(nb, j)
            g_tile(nb - 1, j)
        g_copy(nb - 1).start()

        @pl.loop(0, NS)
        def _(s):
            comm_d(nb, s)
            d_tile(nb - 1, s)

        g_copy(nb - 1).wait()

    nu = nb * NS

    def phase2(xt, gt, ot):
        th = xt.shape[3]
        nv = NS
        tv = Vl // nv
        nt = dw1_hbm.shape[0] // th

        def xt_copy(h):
            cols = pl.ds(pl.multiple_of(h * th, th), th)
            return pltpu.make_async_copy(x_hbm.at[:, :, cols], xt.at[h % 2], xt_sem.at[h % 2])

        def gt_copy(v):
            cols = pl.ds(pl.multiple_of(v * tv, tv), tv)
            return pltpu.make_async_copy(g_hbm.at[:, :, cols], gt.at[:, :, cols], gt_sem.at[v])

        def ot_copy(t):
            h, v = t // nv, t % nv
            return pltpu.make_async_copy(
                ot.at[t % 2],
                dw1_hbm.at[pl.ds(pl.multiple_of(h * th, th), th), pl.ds(pl.multiple_of(v * tv, tv), tv)],
                ot_sem.at[t % 2])

        xt_copy(0).start()
        for v in range(nv):
            gt_copy(v).start()

        @pl.loop(0, nt * nv)
        def _(t):
            h, v = t // nv, t % nv

            @pl.when(t < NS)
            def _():
                comm_z(nb + 1, t)

            @pl.when(jnp.logical_and(t >= 4, t < 6))
            def _():
                u2(nu - 2 + t - 4)

            @pl.when(jnp.logical_and(t >= 7, t < 7 + NS))
            def _():
                u3(nu - NS + t - 7)

            for when_, (step_, k0) in ((1, (ag_a, 3)), (6, (o_wait, 6)), (6, (ag_c, 2)), (6, (ag_b, 3)),
                                       (6, (ag_a, 4)), (6, (ag_a, 5)), (9, (ag_a, 6)),
                                       (12, (o_wait, 7)), (12, (ag_a, 7)), (13, (ag_c, 3)),
                                       (14, (ag_b, 4)), (17, (ag_b, 5)), (19, (ag_b, 6)),
                                       (22, (ag_c, 4)), (22, (ag_b, 7)), (23, (ag_c, 5))):
                @pl.when(t == when_)
                def _(step_=step_, k0=k0):
                    step_(k0)

            @pl.when(v == 0)
            def _():
                xt_copy(h).wait()

            @pl.when(jnp.logical_and(v == 0, h + 1 < nt))
            def _():
                xt_copy(h + 1).start()

            @pl.when(h == 0)
            def _():
                gt_copy(v).wait()

            @pl.when(t >= 2)
            def _():
                ot_copy(t - 2).wait()
            cols = pl.ds(pl.multiple_of(v * tv, tv), tv)
            ot[t % 2] = lax.dot_general(
                xt[h % 2].reshape(T, th), gt[:, :, cols].reshape(T, tv),
                (((0,), (0,)), ((), ())), preferred_element_type=F32).astype(BF16)
            ot_copy(t).start()

        for t in range(nt * nv - 2, nt * nv):
            ot_copy(t).wait()

    vm = pltpu.VMEM
    pl.run_scoped(phase1, vm((H, Vl), BF16), vm((BT, Vl), F32), vm((2, n, R, H), BF16),
                  vm((n, R, Vl), BF16))
    th = TD
    pl.run_scoped(phase2, vm((2, n, own, th), BF16), vm((n, own, Vl), BF16),
                  vm((2, th, Vl // NS), BF16))

    ag_c(6)
    ag_c(7)
    for k in range(nb):
        ag_end(k)
    for u in range(nu - 3, nu):
        d2d_copy(u).wait_send()
    for u in range(nu - 4, nu):
        for d in range(2):
            rs1_copy(u, d).wait_send()
    for u in range(nu - NSL, nu):
        for d in range(2):
            rs2_copy(u, d).wait_send()


def _rest(inv_t, x_hbm, g_hbm, dw1_hbm, dxf_hbm, loss_ref, dw_hbm, dx_hbm, l_ref,
          xt, gt, ot, cb, xt_sem, gt_sem, ot_sem, rd_sem, wr_sem):
    T, H = x_hbm.shape
    Vl = g_hbm.shape[1]
    nv, th = NS, TD
    tv = Vl // nv
    nh = H // th - NT
    rows, nbuf = cb.shape[1], cb.shape[0]
    ahead = nbuf // 2
    ndx = T // rows
    nc = ndx + NT * th // rows
    per = -(-nc // (nh * nv))

    def xt_copy(h):
        cols = pl.ds(pl.multiple_of((h + NT) * th, th), th)
        return pltpu.make_async_copy(x_hbm.at[:, cols], xt.at[h % 2], xt_sem.at[h % 2])

    def gt_copy(v):
        cols = pl.ds(pl.multiple_of(v * tv, tv), tv)
        return pltpu.make_async_copy(g_hbm.at[:, cols], gt.at[:, cols], gt_sem.at[v])

    def ot_copy(t):
        h, v = t // nv, t % nv
        return pltpu.make_async_copy(
            ot.at[t % 2],
            dw_hbm.at[pl.ds(pl.multiple_of((h + NT) * th, th), th), pl.ds(pl.multiple_of(v * tv, tv), tv)],
            ot_sem.at[t % 2])

    def rd_start(c):
        @pl.when(c < ndx)
        def _():
            r = pl.ds(pl.multiple_of(c * rows, rows), rows)
            pltpu.make_async_copy(dxf_hbm.at[r], cb.at[c % nbuf], rd_sem.at[c % nbuf]).start()

        @pl.when(jnp.logical_and(c >= ndx, c < nc))
        def _():
            r = pl.ds(pl.multiple_of((c - ndx) * rows, rows), rows)
            pltpu.make_async_copy(dw1_hbm.at[r], cb.at[c % nbuf], rd_sem.at[c % nbuf]).start()

    def rd_wait(c):
        pltpu.make_async_copy(dxf_hbm.at[pl.ds(0, rows)], cb.at[c % nbuf], rd_sem.at[c % nbuf]).wait()

    def wr_start(c):
        @pl.when(c < ndx)
        def _():
            r = pl.ds(pl.multiple_of(c * rows, rows), rows)
            pltpu.make_async_copy(cb.at[c % nbuf], dx_hbm.at[r], wr_sem.at[c % nbuf]).start()

        @pl.when(c >= ndx)
        def _():
            r = pl.ds(pl.multiple_of((c - ndx) * rows, rows), rows)
            pltpu.make_async_copy(cb.at[c % nbuf], dw_hbm.at[r], wr_sem.at[c % nbuf]).start()

    def wr_wait(c):
        pltpu.make_async_copy(cb.at[c % nbuf], dx_hbm.at[pl.ds(0, rows)], wr_sem.at[c % nbuf]).wait()

    xt_copy(0).start()
    for v in range(nv):
        gt_copy(v).start()
    for c in range(ahead):
        rd_start(c)
    l_ref[0] = jnp.sum(loss_ref[...]) * inv_t

    @pl.loop(0, nh * nv)
    def _(t):
        h, v = t // nv, t % nv

        @pl.loop(0, per)
        def _(q):
            c = t * per + q

            @pl.when(c < nc)
            def _():
                rd_wait(c)
                wr_start(c)

                @pl.when(c >= ahead)
                def _():
                    wr_wait(c - ahead)
                rd_start(c + ahead)

        @pl.when(v == 0)
        def _():
            xt_copy(h).wait()

        @pl.when(jnp.logical_and(v == 0, h + 1 < nh))
        def _():
            xt_copy(h + 1).start()

        @pl.when(h == 0)
        def _():
            gt_copy(v).wait()

        @pl.when(t >= 2)
        def _():
            ot_copy(t - 2).wait()
        cols = pl.ds(pl.multiple_of(v * tv, tv), tv)
        ot[t % 2] = lax.dot_general(xt[h % 2], gt[:, cols], (((0,), (0,)), ((), ())),
                                    preferred_element_type=F32).astype(BF16)
        ot_copy(t).start()

    for t in range(nh * nv - 2, nh * nv):
        ot_copy(t).wait()
    for c in range(nc - ahead, nc):
        wr_wait(c)


def solution(mesh):
    n = mesh.shape["tp"]

    def local(X, W, labels):
        T, H = X.shape
        Vl = W.shape[1]
        own = T // n
        R = 32
        nb = own // R
        BT = n * R
        TH = H // NS
        off = lax.axis_index("tp") * Vl
        lab = jnp.broadcast_to((labels - off)[:, None], (T, LANES)).reshape(n, own, LANES)
        hbm = pl.BlockSpec(memory_space=pl.ANY)
        vm = pltpu.VMEM
        dma = pltpu.SemaphoreType.DMA
        g, dxf, dw1, loss = pl.pallas_call(
            functools.partial(_main, n, nb, T),
            out_shape=(jax.ShapeDtypeStruct((n, own, Vl), BF16),
                       jax.ShapeDtypeStruct((n, own, H), BF16),
                       jax.ShapeDtypeStruct((NT * TD, Vl), BF16),
                       jax.ShapeDtypeStruct((1, BT), F32)),
            in_specs=[hbm, hbm, hbm],
            out_specs=(hbm, hbm, hbm, pl.BlockSpec(memory_space=pltpu.VMEM)),
            scratch_shapes=[
                vm((3, n, R, LANES), jnp.int32),
                vm((BT, LANES), F32), vm((BT, LANES), F32), vm((BT, LANES), F32),
                vm((BT, LANES), F32), vm((BT, LANES), F32),
                vm((2, 8, BT), F32), vm((2, n, 8, BT), F32),
                vm((3, n // 2, 2, R, TH), F32), vm((NSL, n // 2, R, TH), F32),
                vm((NSL, 2, R // 2, TH), F32), vm((NSL, 2, R, TH), F32),
                vm((4, R, TH), F32), vm((NSL, 2, R, TH), F32), vm((NSL, R, TH), F32),
                vm((NS, R, TH), BF16),
                dma((NS,)), dma((2,)), dma((3,)), dma, dma((2, n)), dma((2, n)),
                dma((3,)), dma((NSL,)), dma((4, 2)), dma((NSL, 2)), dma((NSL, 2)),
                dma((NSL, 2)), dma((NS,)),
                dma((8, nb)), dma((8, nb)), dma((2,)), dma((NS,)), dma((2,)),
            ],
            compiler_params=pltpu.CompilerParams(
                collective_id=0, has_side_effects=True, vmem_limit_bytes=67043328),
            cost_estimate=pl.CostEstimate(flops=5 * T * H * Vl,
                                          bytes_accessed=2 * (H * Vl + T * (H + Vl)),
                                          transcendentals=2 * T * Vl),
            name="head_main",
        )(X.reshape(n, own, H), W, lab)
        tv = Vl // NS
        dW, dX, L = pl.pallas_call(
            functools.partial(_rest, 1.0 / T),
            out_shape=(jax.ShapeDtypeStruct((H, Vl), BF16), jax.ShapeDtypeStruct((T, H), BF16),
                       jax.ShapeDtypeStruct((1,), F32)),
            in_specs=[hbm, hbm, hbm, hbm, pl.BlockSpec(memory_space=pltpu.VMEM)],
            out_specs=(hbm, hbm, pl.BlockSpec(memory_space=pltpu.SMEM)),
            scratch_shapes=[vm((2, T, TD), BF16), vm((T, Vl), BF16), vm((2, TD, tv), BF16),
                            vm((16, 128, H), BF16),
                            dma((2,)), dma((NS,)), dma((2,)), dma((16,)), dma((16,))],
            compiler_params=pltpu.CompilerParams(vmem_limit_bytes=56 * 1024 * 1024),
            cost_estimate=pl.CostEstimate(flops=T * H * Vl,
                                          bytes_accessed=2 * (H * Vl + T * (H + Vl)),
                                          transcendentals=0),
            name="head_rest",
        )(X, g.reshape(T, Vl), dw1, dxf.reshape(T, H), loss)
        return L, dW, dX

    return jax.shard_map(local, mesh=mesh,
                         in_specs=(P('dp', None), P(None, 'tp'), P('dp')),
                         out_specs=(P('dp'), P('dp', 'tp'), P('dp', None)),
                         check_vma=False)
```

```python
import functools
import math

import jax
import jax.numpy as jnp
from jax import lax
from jax.experimental import pallas as pl
from jax.experimental.pallas import tpu as pltpu
from jax.sharding import PartitionSpec as P

F32 = jnp.float32
BF16 = jnp.bfloat16
MESH = pl.DeviceIdType.MESH

NS = 4
NSL = 8
LANES = 128
TD = 512
NT = 5


def _main(n, nb, T, x_hbm, w_hbm, lab_ref, g_hbm, dxf_hbm, dw1_hbm, loss_ref,
          lab_v, lab_t, m_s, mr_s, s_s, t_s, mrep, rrep,
          st_send, st_v, dxb, d2d, r1, r2, s1, s2, fin, o_v,
          w_sem, x_sem, g_sem, st_ssem, st_rsem,
          d2d_ssem, d2d_rsem, s1_ssem, r1_rsem, s2_ssem, r2_rsem, o_sem,
          ag_ssem, ag_rsem, xt_sem, gt_sem, ot_sem):
    nch = n // 2
    own = x_hbm.shape[1]
    R = lab_v.shape[2]
    BT = n * R
    H, Vl = w_hbm.shape
    TN = Vl // NS
    TH = H // NS
    inv_t = 1.0 / T
    me = lax.axis_index("tp")
    p, c = me // 2, me % 2
    co = 1 - c
    pr, plf, po = (p + 1) % nch, (p + nch - 1) % nch, (p + 2) % nch
    right, left, partner = {"tp": pr * 2 + c}, {"tp": plf * 2 + c}, {"tp": p * 2 + co}

    def rows_of(b):
        return pl.ds(pl.multiple_of(b * R, R), R)

    def lab_build(b):
        lt = lab_t[rows_of(b), :]
        for q in range(n):
            lab_v[b % 2, q] = jnp.broadcast_to(lt[:, q:q + 1], (R, LANES))

    def st_copy(b, d):
        dev = (me + d) % n
        return pltpu.make_async_remote_copy(
            st_send.at[b % 2], st_v.at[b % 2, me], st_ssem.at[b % 2, d], st_rsem.at[b % 2, d],
            device_id={"tp": dev}, device_id_type=MESH)

    def d2d_copy(u):
        return pltpu.make_async_remote_copy(
            dxb.at[u % 3, :, co], d2d.at[u % NSL], d2d_ssem.at[u % 3], d2d_rsem.at[u % NSL],
            device_id=partner, device_id_type=MESH)

    hr = R // 2

    def rs1_copy(u, d):
        return pltpu.make_async_remote_copy(
            s1.at[u % 4, pl.ds(d * hr, hr)], r1.at[u % NSL, d],
            s1_ssem.at[u % 4, d], r1_rsem.at[u % NSL, d],
            device_id=right if d == 0 else left, device_id_type=MESH)

    def rs2_copy(u, d):
        return pltpu.make_async_remote_copy(
            s2.at[u % NSL, d], r2.at[u % NSL, d], s2_ssem.at[u % NSL, d], r2_rsem.at[u % NSL, d],
            device_id=right if d == 0 else left, device_id_type=MESH)

    def o_copy(u):
        b, s = u // NS, u % NS
        return pltpu.make_async_copy(
            o_v.at[s], dxf_hbm.at[me, rows_of(b), pl.ds(pl.multiple_of(s * TH, TH), TH)],
            o_sem.at[s])

    opp = po * 2 + c
    qr, ql = pr * 2 + c, plf * 2 + c

    def ag_copy(kind, k, owner, lo, rows, dev):
        r = pl.ds(pl.multiple_of(k * R + lo, rows), rows)
        return pltpu.make_async_remote_copy(
            dxf_hbm.at[owner, r], dxf_hbm.at[owner, r], ag_ssem.at[kind, k], ag_rsem.at[kind, k],
            device_id=dev, device_id_type=MESH)

    def ag_all(k):
        args = [(me, 0, R, right), (me, 0, R, left), (me, 0, R, partner),
                (ql, 0, hr, right), (qr, hr, hr, left),
                (ql, 0, R, partner), (qr, 0, R, partner), (opp, 0, R, partner)]
        return [functools.partial(ag_copy, i, k, *x) for i, x in enumerate(args)]

    def ag_a(k):
        cs = ag_all(k)
        for i in (0, 1, 2):
            cs[i]().start()

    def ag_b(k):
        cs = ag_all(k)
        for i in (0, 1):
            cs[i]().wait_recv()
        for i in (3, 4, 5, 6):
            cs[i]().start()

    def ag_c(k):
        cs = ag_all(k)
        for i in (3, 4):
            cs[i]().wait_recv()
        cs[7]().start()

    def ag_end(k):
        cs = ag_all(k)
        for i in (2, 5, 6, 7):
            cs[i]().wait_recv()
        for cp in cs:
            cp().wait_send()

    def u1(u):
        d2d_copy(u).wait_recv()
        k, kd = u % 3, u % NSL

        @pl.when(u >= 4)
        def _():
            for d in range(2):
                rs1_copy(u - 4, d).wait_send()

        @pl.when(u >= NSL)
        def _():
            for d in range(2):
                rs2_copy(u - NSL, d).wait_send()
        s1[u % 4] = dxb[k, po, c] + d2d[kd, po]
        for d in range(2):
            rs1_copy(u, d).start()
        s2[kd, 0] = dxb[k, pr, c] + d2d[kd, pr]
        s2[kd, 1] = dxb[k, plf, c] + d2d[kd, plf]
        fin[kd] = dxb[k, p, c] + d2d[kd, p]

    def u2(u):
        kd = u % NSL
        for d in range(2):
            rs1_copy(u, d).wait_recv()
            half = pl.ds(d * hr, hr)
            s2[kd, d, half] = s2[kd, d, half] + r1[kd, d]
            rs2_copy(u, d).start()

    def u3(u):
        kd = u % NSL
        for d in range(2):
            rs2_copy(u, d).wait_recv()
        o_v[u % NS] = (fin[kd] + r2[kd, 0] + r2[kd, 1]).astype(BF16)
        o_copy(u).start()

    def when(cond):
        return pl.when(cond)

    def o_wait(b):
        for s in range(NS):
            o_copy(b * NS + s).wait()

    def comm_z(i, j):
        @when(jnp.logical_and(j < 2, i >= 2))
        def _():
            u1((i - 2) * NS + 2 + j)

        @when(jnp.logical_and(j < 3, i >= 3))
        def _():
            u3((i - 3) * NS + 1 + j)

        @when(jnp.logical_and(j >= 2, i >= 2))
        def _():
            u2((i - 2) * NS + j - 2)

    def comm_d(i, s):
        @when(jnp.logical_and(s < 2, i >= 2))
        def _():
            u2((i - 2) * NS + 2 + s)

        @when(s >= 2)
        def _():
            u1((i - 1) * NS + s - 2)

        @when(jnp.logical_and(s == 3, i >= 2))
        def _():
            u3((i - 2) * NS)

        @when(jnp.logical_and(s == 2, i >= 3))
        def _():
            o_wait(i - 3)

        @when(jnp.logical_and(s == 2, jnp.logical_and(i >= 5, i % 2 == 1)))
        def _():
            ag_c((i - 5) // 2)

        @when(jnp.logical_and(s == 2, jnp.logical_and(i >= 3, i % 2 == 1)))
        def _():
            ag_a((i - 3) // 2)

        @when(jnp.logical_and(s == 2, jnp.logical_and(i >= 4, i % 2 == 0)))
        def _():
            ag_b((i - 4) // 2)

    lane = lax.broadcasted_iota(jnp.int32, (BT, LANES), 1)

    bar = pltpu.get_barrier_semaphore()
    for d in range(1, n):
        pl.semaphore_signal(bar, inc=1, device_id={"tp": (me + d) % n}, device_id_type=MESH)
    pl.semaphore_wait(bar, n - 1)

    def phase1(w_v, z_v, x_v, g_v):
        def w_copy(j):
            cols = pl.ds(pl.multiple_of(j * TN, TN), TN)
            return pltpu.make_async_copy(w_hbm.at[:, cols], w_v.at[:, cols], w_sem.at[j])

        def x_copy(b):
            return pltpu.make_async_copy(x_hbm.at[:, rows_of(b), :], x_v.at[b % 2], x_sem.at[b % 2])

        def g_copy(b):
            return pltpu.make_async_copy(g_v, g_hbm.at[:, rows_of(b), :], g_sem)

        def z_tile(b, j):
            cols = pl.ds(pl.multiple_of(j * TN, TN), TN)
            z_v[:, cols] = jnp.dot(x_v[b % 2].reshape(BT, H), w_v[:, cols],
                                          preferred_element_type=F32)

        def z_cols(j, rows):
            return [z_v[rows, pl.ds(pl.multiple_of(j * TN + k * LANES, LANES), LANES)]
                    for k in range(TN // LANES)]

        def stat_max(j):
            for r in range(0, BT, 16):
                rows = pl.ds(r, 16)
                m_s[rows] = functools.reduce(jnp.maximum, z_cols(j, rows), m_s[rows])

        def stat_sum(b, j):
            for r in range(0, BT, 16):
                rows = pl.ds(r, 16)
                lab = lab_v[b % 2].reshape(BT, LANES)[r:r + 16]
                ln = lane[r:r + 16]
                m = m_s[rows]
                acc = s_s[rows] * jnp.exp(mr_s[rows] - m)
                tgt = t_s[rows]
                for k, zk in enumerate(z_cols(j, rows)):
                    acc = acc + jnp.exp(zk - m)
                    tgt = tgt + jnp.where(lab == ln + (j * TN + k * LANES), zk, 0.0)
                mr_s[rows] = m
                s_s[rows] = acc
                t_s[rows] = tgt

        def g_tile(b, j):
            rb = 2 * R
            for r in range(0, BT, rb):
                rows = pl.ds(r, rb)
                lab = lab_v[b % 2].reshape(BT, LANES)[r:r + rb]
                ln = lane[r:r + rb]
                mm, rr = mrep[rows], rrep[rows]
                for k in range(TN // LANES):
                    base = pl.multiple_of(j * TN + k * LANES, LANES)
                    z = z_v[rows, pl.ds(base, LANES)]
                    e = jnp.exp(z - mm) * rr
                    g = (e - jnp.where(lab == ln + base, 1.0, 0.0)) * inv_t
                    g_v[pl.ds(r // R, rb // R), :, pl.ds(base, LANES)] = (
                        g.astype(BF16).reshape(rb // R, R, LANES))

        def stats_init():
            m_s[...] = jnp.full((BT, LANES), -jnp.inf, F32)
            mr_s[...] = jnp.full((BT, LANES), -jnp.inf, F32)
            s_s[...] = jnp.zeros((BT, LANES), F32)
            t_s[...] = jnp.zeros((BT, LANES), F32)

        def stats_final(b):
            ml = m_s[...]
            m = jnp.max(ml, axis=1, keepdims=True)
            s = jnp.sum(s_s[...] * jnp.exp(ml - m), axis=1, keepdims=True)
            t = jnp.sum(t_s[...], axis=1, keepdims=True)
            a = jnp.where(lane == 0, m, jnp.where(lane == 1, s, t))
            a = a.T[0:8]
            st_send[b % 2] = a
            st_v[b % 2, me] = a

        def stats_start(b):
            for d in range(1, n):
                st_copy(b, d).start()

        def stats_recv(b):
            k = b % 2
            for d in range(1, n):
                st_copy(b, d).wait()
            ms = st_v[k, :, 0, :]
            m = jnp.max(ms, axis=0, keepdims=True)
            s = jnp.sum(st_v[k, :, 1, :] * jnp.exp(ms - m), axis=0, keepdims=True)
            t = jnp.sum(st_v[k, :, 2, :], axis=0, keepdims=True)
            loss_ref[...] += m + jnp.log(s) - t
            row = lax.broadcasted_iota(jnp.int32, (LANES, BT), 0)
            a = jnp.where(row == 0, m, 1.0 / s).T
            mrep[...] = jnp.broadcast_to(a[:, 0:1], (BT, LANES))
            rrep[...] = jnp.broadcast_to(a[:, 1:2], (BT, LANES))

        def d_free(u):
            @pl.when(u >= 3)
            def _():
                d2d_copy(u - 3).wait_send()

        def d_tile(b, s):
            u = b * NS + s
            gs = g_v[...].reshape(BT, Vl)
            dx = lax.dot_general(gs, w_v[pl.ds(pl.multiple_of(s * TH, TH), TH), :],
                                 (((1,), (1,)), ((), ())), preferred_element_type=F32)
            dxb[u % 3] = dx.reshape(nch, 2, R, TH)
            d2d_copy(u).start()

        for j in range(NS):
            w_copy(j).start()
            if j == 0:
                x_copy(0).start()
                x_copy(1).start()
        loss_ref[...] = jnp.zeros_like(loss_ref)
        stats_init()
        x_copy(0).wait()
        lab_t[...] = jnp.concatenate([lab_ref[...] - me * Vl] * (LANES // n), axis=0).T
        lab_build(0)

        @pl.loop(0, NS)
        def _(j):
            w_copy(j).wait()
            z_tile(0, j)

            @pl.loop(0, 1)
            def _(_):
                stat_max(j)
                stat_sum(0, j)
        stats_final(0)
        stats_start(0)

        @pl.loop(1, nb)
        def _(i):
            x_copy(i).wait()
            lab_build(i)

            @pl.when(i >= 2)
            def _():
                g_copy(i - 2).wait()

            @pl.when(i + 1 < nb)
            def _():
                x_copy(i + 1).start()

            @pl.loop(0, NS)
            def _(j):
                @pl.when(j >= 2)
                def _():
                    stat_sum(i, j - 2)
                comm_z(i, j)

                @pl.when(j == 0)
                def _():
                    stats_recv(i - 1)
                    stats_init()
                    g_tile(i - 1, 0)
                    z_tile(i, 0)

                @pl.when(j >= 1)
                def _():
                    stat_max(j - 1)
                    g_tile(i - 1, j)
                    z_tile(i, j)
            g_copy(i - 1).start()

            @pl.loop(0, NS)
            def _(s):
                comm_d(i, s)
                d_free((i - 1) * NS + s)

                @pl.when(s == 0)
                def _():
                    stat_max(NS - 1)
                    stat_sum(i, NS - 2)
                    stat_sum(i, NS - 1)
                    stats_final(i)
                    d_tile(i - 1, 0)
                    stats_start(i)

                @pl.when(s > 0)
                def _():
                    d_tile(i - 1, s)

        stats_recv(nb - 1)
        g_copy(nb - 2).wait()

        @pl.loop(0, NS)
        def _(j):
            comm_z(nb, j)
            g_tile(nb - 1, j)
        g_copy(nb - 1).start()

        @pl.loop(0, NS)
        def _(s):
            comm_d(nb, s)
            d_free((nb - 1) * NS + s)
            d_tile(nb - 1, s)

        g_copy(nb - 1).wait()

    nu = nb * NS

    def phase2(xt, gt, ot):
        th = xt.shape[3]
        nv = NS
        tv = Vl // nv
        nt = dw1_hbm.shape[0] // th

        def xt_copy(h):
            cols = pl.ds(pl.multiple_of(h * th, th), th)
            return pltpu.make_async_copy(x_hbm.at[:, :, cols], xt.at[h % 2], xt_sem.at[h % 2])

        def gt_copy(v):
            cols = pl.ds(pl.multiple_of(v * tv, tv), tv)
            return pltpu.make_async_copy(g_hbm.at[:, :, cols], gt.at[:, :, cols], gt_sem.at[v])

        def ot_copy(t):
            h, v = t // nv, t % nv
            return pltpu.make_async_copy(
                ot.at[t % 2],
                dw1_hbm.at[pl.ds(pl.multiple_of(h * th, th), th), pl.ds(pl.multiple_of(v * tv, tv), tv)],
                ot_sem.at[t % 2])

        xt_copy(0).start()
        for v in range(nv):
            gt_copy(v).start()

        @pl.loop(0, nt * nv)
        def _(t):
            h, v = t // nv, t % nv

            @pl.when(t < NS)
            def _():
                comm_z(nb + 1, t)

            @pl.when(jnp.logical_and(t >= 4, t < 6))
            def _():
                u2(nu - 2 + t - 4)

            @pl.when(jnp.logical_and(t >= 7, t < 7 + NS))
            def _():
                u3(nu - NS + t - 7)

            for when_, (step_, k0) in ((1, (ag_a, 3)), (6, (o_wait, 6)), (6, (ag_c, 2)), (6, (ag_b, 3)),
                                       (6, (ag_a, 4)), (6, (ag_a, 5)), (9, (ag_a, 6)),
                                       (12, (o_wait, 7)), (12, (ag_a, 7)), (13, (ag_c, 3)),
                                       (14, (ag_b, 4)), (17, (ag_b, 5)), (19, (ag_b, 6)),
                                       (19, (ag_c, 4)), (19, (ag_b, 7)), (19, (ag_c, 5))):
                @pl.when(t == when_)
                def _(step_=step_, k0=k0):
                    step_(k0)

            @pl.when(v == 0)
            def _():
                xt_copy(h).wait()

            @pl.when(jnp.logical_and(v == 0, h + 1 < nt))
            def _():
                xt_copy(h + 1).start()

            @pl.when(h == 0)
            def _():
                gt_copy(v).wait()

            @pl.when(t >= 2)
            def _():
                ot_copy(t - 2).wait()
            cols = pl.ds(pl.multiple_of(v * tv, tv), tv)
            ot[t % 2] = lax.dot_general(
                xt[h % 2].reshape(T, th), gt[:, :, cols].reshape(T, tv),
                (((0,), (0,)), ((), ())), preferred_element_type=F32).astype(BF16)
            ot_copy(t).start()

        for t in range(nt * nv - 2, nt * nv):
            ot_copy(t).wait()

    vm = pltpu.VMEM
    pl.run_scoped(phase1, vm((H, Vl), BF16), vm((BT, Vl), F32), vm((2, n, R, H), BF16),
                  vm((n, R, Vl), BF16))
    th = TD
    pl.run_scoped(phase2, vm((2, n, own, th), BF16), vm((n, own, Vl), BF16),
                  vm((2, th, Vl // NS), BF16))

    ag_c(6)
    ag_c(7)
    for k in range(nb):
        ag_end(k)
    for u in range(nu - 3, nu):
        d2d_copy(u).wait_send()
    for u in range(nu - 4, nu):
        for d in range(2):
            rs1_copy(u, d).wait_send()
    for u in range(nu - NSL, nu):
        for d in range(2):
            rs2_copy(u, d).wait_send()


def _rest(inv_t, x_hbm, g_hbm, dw1_hbm, dxf_hbm, loss_ref, dw_hbm, dx_hbm, l_ref,
          xt, gt, ot, cb, xt_sem, gt_sem, ot_sem, rd_sem, wr_sem):
    T, H = x_hbm.shape
    Vl = g_hbm.shape[1]
    nv, th = NS, TD
    tv = Vl // nv
    nh = H // th - NT
    rows, nbuf = cb.shape[1], cb.shape[0]
    ahead = nbuf // 2
    ndx = T // rows
    nc = ndx + NT * th // rows
    per = -(-nc // (nh * nv))

    def xt_copy(h):
        cols = pl.ds(pl.multiple_of((h + NT) * th, th), th)
        return pltpu.make_async_copy(x_hbm.at[:, cols], xt.at[h % 2], xt_sem.at[h % 2])

    def gt_copy(v):
        cols = pl.ds(pl.multiple_of(v * tv, tv), tv)
        return pltpu.make_async_copy(g_hbm.at[:, cols], gt.at[:, cols], gt_sem.at[v])

    def ot_copy(t):
        h, v = t // nv, t % nv
        return pltpu.make_async_copy(
            ot.at[t % 2],
            dw_hbm.at[pl.ds(pl.multiple_of((h + NT) * th, th), th), pl.ds(pl.multiple_of(v * tv, tv), tv)],
            ot_sem.at[t % 2])

    def rd_start(c):
        @pl.when(c < ndx)
        def _():
            r = pl.ds(pl.multiple_of(c * rows, rows), rows)
            pltpu.make_async_copy(dxf_hbm.at[r], cb.at[c % nbuf], rd_sem.at[c % nbuf]).start()

        @pl.when(jnp.logical_and(c >= ndx, c < nc))
        def _():
            r = pl.ds(pl.multiple_of((c - ndx) * rows, rows), rows)
            pltpu.make_async_copy(dw1_hbm.at[r], cb.at[c % nbuf], rd_sem.at[c % nbuf]).start()

    def rd_wait(c):
        pltpu.make_async_copy(dxf_hbm.at[pl.ds(0, rows)], cb.at[c % nbuf], rd_sem.at[c % nbuf]).wait()

    def wr_start(c):
        @pl.when(c < ndx)
        def _():
            r = pl.ds(pl.multiple_of(c * rows, rows), rows)
            pltpu.make_async_copy(cb.at[c % nbuf], dx_hbm.at[r], wr_sem.at[c % nbuf]).start()

        @pl.when(c >= ndx)
        def _():
            r = pl.ds(pl.multiple_of((c - ndx) * rows, rows), rows)
            pltpu.make_async_copy(cb.at[c % nbuf], dw_hbm.at[r], wr_sem.at[c % nbuf]).start()

    def wr_wait(c):
        pltpu.make_async_copy(cb.at[c % nbuf], dx_hbm.at[pl.ds(0, rows)], wr_sem.at[c % nbuf]).wait()

    xt_copy(0).start()
    gt_copy(0).start()
    for v in range(1, nv):
        gt_copy(v).start()
        for c in range(ahead * (v - 1) // (nv - 1), ahead * v // (nv - 1)):
            rd_start(c)
    l_ref[0] = jnp.sum(loss_ref[...]) * inv_t

    @pl.loop(0, nh * nv)
    def _(t):
        h, v = t // nv, t % nv

        @pl.when(v == 0)
        def _():
            xt_copy(h).wait()

        @pl.when(jnp.logical_and(v == 0, h + 1 < nh))
        def _():
            xt_copy(h + 1).start()

        @pl.when(h == 0)
        def _():
            gt_copy(v).wait()

        @pl.when(t >= 2)
        def _():
            ot_copy(t - 2).wait()
        cols = pl.ds(pl.multiple_of(v * tv, tv), tv)
        ot[t % 2] = lax.dot_general(xt[h % 2], gt[:, cols], (((0,), (0,)), ((), ())),
                                    preferred_element_type=F32).astype(BF16)
        ot_copy(t).start()

        @pl.loop(0, per)
        def _(q):
            c = t * per + q

            @pl.when(c < nc)
            def _():
                rd_wait(c)
                wr_start(c)

                @pl.when(c >= ahead)
                def _():
                    wr_wait(c - ahead)
                rd_start(c + ahead)

    for t in range(nh * nv - 2, nh * nv):
        ot_copy(t).wait()
    for c in range(nc - ahead, nc):
        wr_wait(c)


def solution(mesh):
    n = mesh.shape["tp"]

    def local(X, W, labels):
        T, H = X.shape
        Vl = W.shape[1]
        own = T // n
        R = 32
        nb = own // R
        BT = n * R
        TH = H // NS
        lab = labels.reshape(n, own)
        hbm = pl.BlockSpec(memory_space=pl.ANY)
        vm = pltpu.VMEM
        dma = pltpu.SemaphoreType.DMA
        g, dxf, dw1, loss = pl.pallas_call(
            functools.partial(_main, n, nb, T),
            out_shape=(jax.ShapeDtypeStruct((n, own, Vl), BF16),
                       jax.ShapeDtypeStruct((n, own, H), BF16),
                       jax.ShapeDtypeStruct((NT * TD, Vl), BF16),
                       jax.ShapeDtypeStruct((1, BT), F32)),
            in_specs=[hbm, hbm, pl.BlockSpec(memory_space=pltpu.VMEM)],
            out_specs=(hbm, hbm, hbm, pl.BlockSpec(memory_space=pltpu.VMEM)),
            scratch_shapes=[
                vm((2, n, R, LANES), jnp.int32), vm((own, LANES), jnp.int32),
                vm((BT, LANES), F32), vm((BT, LANES), F32), vm((BT, LANES), F32),
                vm((BT, LANES), F32), vm((BT, LANES), F32), vm((BT, LANES), F32),
                vm((2, 8, BT), F32), vm((2, n, 8, BT), F32),
                vm((3, n // 2, 2, R, TH), F32), vm((NSL, n // 2, R, TH), F32),
                vm((NSL, 2, R // 2, TH), F32), vm((NSL, 2, R, TH), F32),
                vm((4, R, TH), F32), vm((NSL, 2, R, TH), F32), vm((NSL, R, TH), F32),
                vm((NS, R, TH), BF16),
                dma((NS,)), dma((2,)), dma, dma((2, n)), dma((2, n)),
                dma((3,)), dma((NSL,)), dma((4, 2)), dma((NSL, 2)), dma((NSL, 2)),
                dma((NSL, 2)), dma((NS,)),
                dma((8, nb)), dma((8, nb)), dma((2,)), dma((NS,)), dma((2,)),
            ],
            compiler_params=pltpu.CompilerParams(
                collective_id=0, has_side_effects=True, vmem_limit_bytes=67043328),
            cost_estimate=pl.CostEstimate(flops=5 * T * H * Vl,
                                          bytes_accessed=2 * (H * Vl + T * (H + Vl)),
                                          transcendentals=2 * T * Vl),
            name="head_main",
        )(X.reshape(n, own, H), W, lab)
        tv = Vl // NS
        dW, dX, L = pl.pallas_call(
            functools.partial(_rest, 1.0 / T),
            out_shape=(jax.ShapeDtypeStruct((H, Vl), BF16), jax.ShapeDtypeStruct((T, H), BF16),
                       jax.ShapeDtypeStruct((1,), F32)),
            in_specs=[hbm, hbm, hbm, hbm, pl.BlockSpec(memory_space=pltpu.VMEM)],
            out_specs=(hbm, hbm, pl.BlockSpec(memory_space=pltpu.SMEM)),
            scratch_shapes=[vm((2, T, TD), BF16), vm((T, Vl), BF16), vm((2, TD, tv), BF16),
                            vm((16, 128, H), BF16),
                            dma((2,)), dma((NS,)), dma((2,)), dma((16,)), dma((16,))],
            compiler_params=pltpu.CompilerParams(vmem_limit_bytes=56 * 1024 * 1024),
            cost_estimate=pl.CostEstimate(flops=T * H * Vl,
                                          bytes_accessed=2 * (H * Vl + T * (H + Vl)),
                                          transcendentals=0),
            name="head_rest",
        )(X, g.reshape(T, Vl), dw1, dxf.reshape(T, H), loss)
        return L, dW, dX

    return jax.shard_map(local, mesh=mesh,
                         in_specs=(P('dp', None), P(None, 'tp'), P('dp')),
                         out_specs=(P('dp'), P('dp', 'tp'), P('dp', None)),
                         check_vma=False)
```
